32 devices in a mesh: row: 4 (over x, core), col: 8 (over z, y).
Axes of the slice: x: 2, y: 2, z: 4, core: 2. Of those that a mesh axis runs over, the one named last changes fastest.
Arguments:
- homolog_trait_tensor: bfloat16 [192, 8192], P(None, ('row', 'col')), may hold values from -6 to 6
- whitening_multiplier: float32 [64], replicated, may hold values from 0.1 to 1.9
- lefthand_projection: bfloat16 [64, 32], replicated, may hold values from -0.75 to 0.75
- righthand_projection: bfloat16 [64, 32], replicated, may hold values from -0.75 to 0.75
- result_matrix: bfloat16 [1024, 128], replicated, may hold values from -0.75 to 0.75
- result_offset: float32 [128], replicated, may hold values from -3 to 3
- sequence_tallies: int32 [16], replicated, may hold values from 64 to 192
- position_molecule: int32 [128], replicated, may hold values from 0 to 15, never falling along the last dimension, each value on 1 to 16 neighbouring positions
- upstream_adjoint: bfloat16 [128, 128, 128], P('row', 'col'), may hold values from -6 to 6
Outputs:
- couple_update_tensor: bfloat16 [128, 128, 128], P('row', 'col')
- homolog_slope_tensor: float32 [192, 8192], P(None, ('row', 'col'))
- grad_w_out: float32 [1024, 128], replicated
The draws below stay inside these ranges and needn't reach their ends.
Inputs may be any that keep to these rules, and one draw needn't show every extreme that they name: `position_molecule`: chain numbers never fall along the residues.
All inputs are finite; a program needn't handle non-finite values.
Results may differ from the reference program's by a relative error of at most 0.006.
Values may be sent and summed in bfloat16 or wider, within the bound.
A program may use at most 128 MiB of HBM per device.

```python
import math
import jax
import jax.numpy as jnp
import numpy as np
from jax import lax

TRAIT_BREADTH = 64
LATENT_CARDINAL = 32
PAIR_CHANNELS = 128
HOMOLOG_TOTALITY = 192
CHAIN_COUNT = 16
SPAN_SITES = 128


def touch_ends(values, stream_key, low, high):
    extent = values.shape
    index_at = [jax.random.randint(jax.random.fold_in(stream_key, axis), (), 0, extent[axis]) for axis in range(len(extent))]
    values = values.at[tuple(index_at)].set(low)
    longest = extent.index(max(extent))
    index_at[longest] = (index_at[longest] + 1) % extent[longest]
    return values.at[tuple(index_at)].set(high)


def level_of(key, extent, pieces, smallest, top_value):
    factor_of, own = 1.0, jax.random.fold_in(key, 6)
    for dim, parts in pieces:
        heights = jnp.exp(jax.random.uniform(jax.random.fold_in(own, dim), (parts,), jnp.float32, smallest / len(pieces), top_value / len(pieces)))
        factor_of = factor_of * jnp.repeat(heights, extent[dim] // parts).reshape([-1 if axis == dim else 1 for axis in range(len(extent))])
    return factor_of


def profile(count, total, limit, skew):
    loads = [(1 << 20) // math.isqrt(standing ** skew) + 1 for standing in range(2, count + 1)]
    spare, given = total - limit - (count - 1), [1] * (count - 1)
    while spare > 0:
        candidates = [i for i in range(count - 1) if given[i] < limit]
        whole, budget = sum([loads[i] for i in candidates]), spare
        for i in candidates:
            more = min(limit - given[i], max(1, budget * loads[i] // whole), spare)
            given[i] = given[i] + more
            spare = spare - more
    return np.array([limit] + given)


def ragged_sizes(own_key, amount, total, bound, skew):
    if amount == 2:
        one = jax.random.randint(own_key, (), max(1, total - bound), min(bound, total - 1) + 1)
        return jnp.stack([one, total - one])
    tallies = jnp.asarray(profile(amount, total, bound, skew), jnp.int32)
    couples = (amount - 1) // 2
    giver, sink = tallies[1:1 + 2 * couples:2], tallies[2:2 + 2 * couples:2]
    margin = jnp.minimum(giver - 1, bound - sink)
    passed = jax.random.randint(jax.random.fold_in(own_key, 1), (couples,), 0, 1 << 20) % (margin + 1)
    tallies = tallies.at[1:1 + 2 * couples:2].set(giver - passed).at[2:2 + 2 * couples:2].set(sink + passed)
    return tallies[jax.random.permutation(jax.random.fold_in(own_key, 2), amount)]


def scatter_about(stream_key, dims, deviation, limit, shards=(), kind=jnp.bfloat16):
    drawn = jax.random.normal(stream_key, dims, jnp.float32) * deviation
    if len(shards) > 0:
        drawn = level_of(stream_key, dims, shards, -0.22, 0.18) * drawn
    return jnp.clip(drawn, min=-limit, max=limit).astype(kind)


def setup_inputs(seed: int = 0) -> dict:
    key_of = jax.random.split(jax.random.key(seed), 10)
    homolog_trait_tensor = scatter_about(key_of[0], (HOMOLOG_TOTALITY, SPAN_SITES * TRAIT_BREADTH), 1.0, 6.0, ((1, 32),))
    whitening_multiplier = jnp.clip(1.0 + 0.18 * jax.random.normal(key_of[1], (TRAIT_BREADTH,), jnp.float32), 0.1, 1.9)
    lefthand_projection = scatter_about(key_of[2], (TRAIT_BREADTH, LATENT_CARDINAL), TRAIT_BREADTH ** -0.5, 0.75)
    righthand_projection = scatter_about(key_of[3], (TRAIT_BREADTH, LATENT_CARDINAL), TRAIT_BREADTH ** -0.5, 0.75)
    result_matrix = scatter_about(key_of[4], (LATENT_CARDINAL * LATENT_CARDINAL, PAIR_CHANNELS), (2 * LATENT_CARDINAL) ** -0.5, 0.75)
    result_offset = scatter_about(key_of[5], (PAIR_CHANNELS,), 0.5, 3.0, (), jnp.float32)
    sequence_tallies = touch_ends(jax.random.randint(key_of[6], (CHAIN_COUNT,), max(1, HOMOLOG_TOTALITY // 3), HOMOLOG_TOTALITY + 1), jax.random.fold_in(key_of[6], 1), max(1, HOMOLOG_TOTALITY // 3), HOMOLOG_TOTALITY).astype(jnp.int32)
    position_molecule = jnp.searchsorted(jnp.cumsum(ragged_sizes(key_of[7], CHAIN_COUNT, SPAN_SITES, 2 * SPAN_SITES // CHAIN_COUNT, 2)), jnp.arange(SPAN_SITES), side="right").astype(jnp.int32)
    upstream_adjoint = scatter_about(key_of[8], (SPAN_SITES, SPAN_SITES, PAIR_CHANNELS), 1.0, 6.0, ((0, 4), (1, 8)))
    return dict(homolog_trait_tensor=homolog_trait_tensor, whitening_multiplier=whitening_multiplier, lefthand_projection=lefthand_projection, righthand_projection=righthand_projection, result_matrix=result_matrix, result_offset=result_offset, sequence_tallies=sequence_tallies, position_molecule=position_molecule, upstream_adjoint=upstream_adjoint)


EPS_NORM = 1e-05
EPS_COUNT = 0.001

def residue_depths(sequence_tallies, position_molecule, chains):
    table = position_molecule[:, None] == jnp.arange(chains, dtype=jnp.int32)[None, :]
    return lax.optimization_barrier(jnp.sum(jnp.where(table, sequence_tallies[None, :], 0), axis=1)).astype(jnp.int32)

def reference(homolog_trait_tensor, whitening_multiplier, lefthand_projection, righthand_projection, result_matrix, result_offset, sequence_tallies, position_molecule, upstream_adjoint):
    exact_precision = lax.Precision.HIGHEST
    operand_tensors = homolog_trait_tensor.astype(jnp.float32).reshape(HOMOLOG_TOTALITY, SPAN_SITES, TRAIT_BREADTH)
    centred = operand_tensors - lax.optimization_barrier(jnp.mean(operand_tensors, axis=-1, keepdims=True))
    inverse_deviation = lax.rsqrt(lax.optimization_barrier(jnp.mean(centred * centred, axis=-1, keepdims=True)) + EPS_NORM)
    normalized_alignment = centred * inverse_deviation
    scaled_features = normalized_alignment * whitening_multiplier
    residue_row_depth = residue_depths(sequence_tallies, position_molecule, CHAIN_COUNT)
    depth_mask = (jnp.arange(HOMOLOG_TOTALITY, dtype=jnp.int32)[:, None] < residue_row_depth[None, :]).astype(jnp.float32)
    left_projected = (jnp.einsum('yel,lr->yer', scaled_features, lefthand_projection.astype(jnp.float32), precision=exact_precision) * depth_mask[:, :, None]).astype(jnp.bfloat16).reshape(HOMOLOG_TOTALITY, SPAN_SITES * LATENT_CARDINAL)
    right_projected = (jnp.einsum('yel,lr->yer', scaled_features, righthand_projection.astype(jnp.float32), precision=exact_precision) * depth_mask[:, :, None]).astype(jnp.bfloat16).reshape(HOMOLOG_TOTALITY, SPAN_SITES * LATENT_CARDINAL)
    counts = jnp.dot(depth_mask.T, depth_mask, precision=exact_precision) + EPS_COUNT
    step_rows = 16

    def one_block(carried, block_index):
        coverage_tally_total, right_accumulated_sum = carried
        start = block_index * step_rows
        left_block = lax.dynamic_slice_in_dim(left_projected, start * LATENT_CARDINAL, step_rows * LATENT_CARDINAL, 1)
        divisor = lax.dynamic_slice_in_dim(counts, start, step_rows, 0)[:, :, None]
        product = lax.dot_general(left_block, right_projected, (((0,), (0,)), ((), ())), preferred_element_type=jnp.float32)
        outer = product.reshape(step_rows, LATENT_CARDINAL, SPAN_SITES, LATENT_CARDINAL).transpose(0, 2, 1, 3).reshape(step_rows, SPAN_SITES, LATENT_CARDINAL * LATENT_CARDINAL)
        outer = (outer / divisor).astype(jnp.bfloat16)
        flat = outer.reshape(step_rows * SPAN_SITES, LATENT_CARDINAL * LATENT_CARDINAL)
        update = (jnp.dot(flat, result_matrix, preferred_element_type=jnp.float32) + result_offset).astype(jnp.bfloat16)
        update = update.reshape(step_rows, SPAN_SITES, PAIR_CHANNELS)
        incoming = lax.dynamic_slice_in_dim(upstream_adjoint, start, step_rows, 0).reshape(step_rows * SPAN_SITES, PAIR_CHANNELS)
        coverage_tally_total = coverage_tally_total + jnp.dot(flat.T, incoming, preferred_element_type=jnp.float32)
        grad_outer = jnp.dot(incoming, result_matrix.T, preferred_element_type=jnp.float32).reshape(step_rows, SPAN_SITES, LATENT_CARDINAL * LATENT_CARDINAL)
        grad_outer = (grad_outer / divisor).astype(jnp.bfloat16)
        grad_matrix = grad_outer.reshape(step_rows, SPAN_SITES, LATENT_CARDINAL, LATENT_CARDINAL).transpose(0, 2, 1, 3).reshape(step_rows * LATENT_CARDINAL, SPAN_SITES * LATENT_CARDINAL)
        left_grad = lax.dot_general(right_projected, grad_matrix, (((1,), (1,)), ((), ())), preferred_element_type=jnp.float32)
        right_accumulated_sum = right_accumulated_sum + jnp.dot(left_block, grad_matrix, preferred_element_type=jnp.float32)
        return ((coverage_tally_total, right_accumulated_sum), (update, left_grad))
    initial_state = (jnp.zeros((LATENT_CARDINAL * LATENT_CARDINAL, PAIR_CHANNELS), jnp.float32), jnp.zeros((HOMOLOG_TOTALITY, SPAN_SITES * LATENT_CARDINAL), jnp.float32))
    (coverage_tally_total, right_accumulated_sum), (updates, left_gradient_rows) = lax.scan(one_block, initial_state, jnp.arange(SPAN_SITES // step_rows, dtype=jnp.int32))
    couple_update_tensor = updates.reshape(SPAN_SITES, SPAN_SITES, PAIR_CHANNELS)
    left_grand_total = left_gradient_rows.transpose(1, 0, 2).reshape(HOMOLOG_TOTALITY, SPAN_SITES, LATENT_CARDINAL) * depth_mask[:, :, None]
    right_grand_total = right_accumulated_sum.reshape(HOMOLOG_TOTALITY, SPAN_SITES, LATENT_CARDINAL) * depth_mask[:, :, None]
    grad_scaled = jnp.einsum('snh,ch->snc', left_grand_total, lefthand_projection.astype(jnp.float32), precision=exact_precision)
    grad_scaled = grad_scaled + jnp.einsum('snh,ch->snc', right_grand_total, righthand_projection.astype(jnp.float32), precision=exact_precision)
    normed_gradient = grad_scaled * whitening_multiplier
    homolog_slope_tensor = inverse_deviation * (normed_gradient - lax.optimization_barrier(jnp.mean(normed_gradient, axis=-1, keepdims=True)) - normalized_alignment * lax.optimization_barrier(jnp.mean(normed_gradient * normalized_alignment, axis=-1, keepdims=True)))
    return (couple_update_tensor, homolog_slope_tensor.reshape(HOMOLOG_TOTALITY, SPAN_SITES * TRAIT_BREADTH), coverage_tally_total / SPAN_SITES)
```

```python
import functools

import jax
import jax.numpy as jnp
from jax import lax
from jax.experimental import pallas as pl
from jax.experimental.pallas import tpu as pltpu
from jax.sharding import PartitionSpec as P

EPS_NORM = 1e-05
EPS_COUNT = 0.001
LANES = 128
BLOCK = 32

f32 = jnp.float32
bf16 = jnp.bfloat16


def dotf(a, b, dims):
    return lax.dot_general(a, b, (dims, ((), ())), preferred_element_type=f32)


def dot_exact(a, b, dims):
    first = a.astype(bf16)
    rest = a - first.astype(f32)
    second = rest.astype(bf16)
    third = (rest - second.astype(f32)).astype(bf16)
    return dotf(third, b, dims) + dotf(second, b, dims) + dotf(first, b, dims)


NN = ((1,), (0,))
NT = ((1,), (1,))
TN = ((0,), (0,))


def kernel(
    n_row, n_col, hidden, embed,
    x_ref, gain_ref, proj_ref, w_ref, offset_ref, depth_ref, recip_ref, adj_ref,
    upd_ref, slope_ref, gw_out_ref,
    normed_ref, inv_ref, lsend_ref, rsend_ref, lall_ref, rall_ref, prod_ref, flat_ref,
    adjf_ref, adjt_ref, updf_ref, gacc_ref, gwsend_ref, w1_ref, w2_ref, w3_ref,
    go_ref, gm_ref, glsend_ref, gracc_ref, grsend_ref, gl_ref, gr_ref,
    ls_sem, lr_sem, rs_sem, rr_sem, gls_sem, glr_sem, grs_sem, grr_sem,
    w1s_sem, w1r_sem, w2s_sem, w2r_sem, w3s_sem, w3r_sem,
):
    r = lax.axis_index("row")
    c = lax.axis_index("col")
    group = n_col // n_row
    depth_s = x_ref.shape[0]
    width = lsend_ref.shape[1]
    per_vreg = LANES // hidden
    left_extent = recip_ref.shape[0]
    right_extent = recip_ref.shape[1] // hidden
    chunks = left_extent // BLOCK
    channels = hidden * hidden
    total = n_row * n_col * (x_ref.shape[1] // embed)

    to_col = r * group + c // n_row
    to_slot = lax.rem(c, n_row)
    own_row = c // group
    own_col = lax.rem(c, group) * n_row
    loops_back = to_col == c

    barrier = pltpu.get_barrier_semaphore()

    def greet(row, col):
        pl.semaphore_signal(
            barrier, inc=1, device_id=(row, col), device_id_type=pl.DeviceIdType.MESH
        )

    for o in range(1, n_col):
        greet(r, lax.rem(c + o, n_col))
    for o in range(1, n_row):
        greet(lax.rem(r + o, n_row), c)
    for k in range(n_row):
        self_target = loops_back & (r == k)
        self_owner = (own_row == r) & (own_col + k == c)

        @pl.when(jnp.logical_not(self_target))
        def _():
            greet(k, to_col)

        @pl.when(jnp.logical_not(self_owner))
        def _():
            greet(own_row, own_col + k)

    def remote(src, dst, send_sem, recv_sem, row, col):
        return pltpu.make_async_remote_copy(
            src_ref=src, dst_ref=dst, send_sem=send_sem, recv_sem=recv_sem,
            device_id=(row, col), device_id_type=pl.DeviceIdType.MESH,
        )

    full = x_ref.shape[1]
    same = (
        lax.broadcasted_iota(jnp.int32, (full, full), 0) // embed
        == lax.broadcasted_iota(jnp.int32, (full, full), 1) // embed
    )
    averager = jnp.where(same, 1.0 / embed, 0.0).astype(bf16)
    x = x_ref[...]
    centred = x.astype(f32) - dotf(x, averager, NN)
    inv = lax.rsqrt(dot_exact(centred * centred, averager, NN) + EPS_NORM)
    normed = centred * inv
    normed_ref[...] = normed
    inv_ref[...] = inv
    gain = gain_ref[...]
    keep = (
        lax.broadcasted_iota(jnp.int32, (depth_s, width), 0) < depth_ref[...]
    ).astype(f32)
    both = dot_exact(normed * gain, proj_ref[...], NN)
    left = (both[:, :width] * keep).astype(bf16)
    right = (both[:, width:] * keep).astype(bf16)
    rsend_ref[...] = right
    lsend_ref[...] = left

    def panel(ref, index):
        return ref.at[:, pl.ds(pl.multiple_of(index * width, LANES), width)]

    pl.semaphore_wait(
        barrier, n_col - 1 + n_row - 1 + 2 * n_row - 2 * loops_back.astype(jnp.int32)
    )

    def left_copy(o):
        return remote(
            lsend_ref, panel(lall_ref, c), ls_sem.at[o], lr_sem.at[c],
            r, lax.rem(c + o, n_col),
        )

    def right_copy(k):
        return remote(
            rsend_ref, panel(rall_ref, to_slot), rs_sem.at[k], rr_sem.at[to_slot], k, to_col
        )

    for k in range(n_row):
        self_target = loops_back & (r == k)

        @pl.when(jnp.logical_not(self_target))
        def _():
            right_copy(k).start()

    for o in range(1, n_col):
        left_copy(o).start()

    @pl.when(loops_back & (r == own_row))
    def _():
        panel(rall_ref, to_slot)[...] = rsend_ref[...]

    panel(lall_ref, c)[...] = left

    rows = BLOCK * right_extent
    for b in range(chunks):
        adjf_ref[...] = adj_ref[b * rows : (b + 1) * rows, :].astype(f32)
        for j in range(right_extent):
            adjt_ref[b * rows + j * BLOCK : b * rows + (j + 1) * BLOCK, :] = adjf_ref[
                pl.ds(j, BLOCK, stride=right_extent), :
            ].astype(bf16)

    for k in range(n_row):
        self_owner = (own_row == r) & (own_col + k == c)

        @pl.when(jnp.logical_not(self_owner))
        def _():
            remote(
                rsend_ref, panel(rall_ref, k), rs_sem.at[k], rr_sem.at[k], own_row, own_col + k
            ).wait_recv()

    for o in range(1, n_col):
        source = lax.rem(c + o, n_col)
        remote(
            lsend_ref, panel(lall_ref, source), ls_sem.at[o], lr_sem.at[source], r, source
        ).wait_recv()

    lane_part = lax.broadcasted_iota(jnp.int32, (BLOCK, LANES), 1) // hidden
    groups_j = right_extent // per_vreg
    groups_h = hidden // per_vreg

    def regroup(tiles, own):
        merged = None
        for t in range(per_vreg):
            shift = ((t - own) * hidden) % LANES
            moved = pltpu.roll(tiles[t], shift, 1) if shift else tiles[t]
            merged = moved if merged is None else jnp.where(lane_part == t, moved, merged)
        return merged

    span = BLOCK * hidden
    gacc_ref[...] = jnp.zeros_like(gacc_ref)

    def forward(b, _):
        start = pl.multiple_of(b * rows, rows)
        recip = recip_ref[pl.ds(pl.multiple_of(b * BLOCK, BLOCK), BLOCK), :]
        left_block = lall_ref[:, pl.ds(pl.multiple_of(b * span, span), span)]
        product = dotf(left_block, rall_ref[...], TN)
        for jq in range(groups_j):
            prod_ref[jq] = product[:, jq * LANES : (jq + 1) * LANES]
        for hq in range(groups_h):
            for jq in range(groups_j):
                scale = recip[:, jq * LANES : (jq + 1) * LANES]
                tiles = [
                    prod_ref[jq, pl.ds(hq * per_vreg + t, BLOCK, stride=hidden), :] * scale
                    for t in range(per_vreg)
                ]
                for jj in range(per_vreg):
                    j = jq * per_vreg + jj
                    flat_ref[
                        j * BLOCK : (j + 1) * BLOCK, hq * LANES : (hq + 1) * LANES
                    ] = regroup(tiles, jj).astype(bf16)
        flat = flat_ref[...]
        incoming = adjt_ref[pl.ds(start, rows), :]
        gacc_ref[...] += dotf(incoming, flat, TN)
        update = dotf(flat, w_ref[...], NN) + offset_ref[...]
        for j in range(right_extent):
            updf_ref[pl.ds(j, BLOCK, stride=right_extent), :] = update[
                j * BLOCK : (j + 1) * BLOCK, :
            ]
        upd_ref[pl.ds(start, rows), :] = updf_ref[...].astype(bf16)
        return 0

    lax.fori_loop(0, chunks, forward, 0)

    piece = channels // n_col
    gwsend_ref[...] = gacc_ref[...].T.astype(bf16)

    def w_rows(ref, index):
        return ref.at[pl.ds(pl.multiple_of(index * piece, piece), piece), :]

    def w1_copy(o):
        target = lax.rem(c + o, n_col)
        return remote(
            w_rows(gwsend_ref, target), w1_ref.at[c], w1s_sem.at[o], w1r_sem.at[c], r, target
        )

    for o in range(1, n_col):
        w1_copy(o).start()
    w1_ref[c] = w_rows(gwsend_ref, c)[...]

    gracc_ref[...] = jnp.zeros_like(gracc_ref)

    def backward(b, _):
        start = pl.multiple_of(b * rows, rows)
        recip = recip_ref[pl.ds(pl.multiple_of(b * BLOCK, BLOCK), BLOCK), :]
        left_block = lall_ref[:, pl.ds(pl.multiple_of(b * span, span), span)]
        go_ref[...] = dotf(adjt_ref[pl.ds(start, rows), :], w_ref[...], NT)
        for hq in range(groups_h):
            for jq in range(groups_j):
                scale = recip[:, jq * LANES : (jq + 1) * LANES]
                tiles = [
                    go_ref[
                        (jq * per_vreg + t) * BLOCK : (jq * per_vreg + t + 1) * BLOCK,
                        hq * LANES : (hq + 1) * LANES,
                    ]
                    for t in range(per_vreg)
                ]
                for hh in range(per_vreg):
                    gm_ref[jq, pl.ds(hq * per_vreg + hh, BLOCK, stride=hidden), :] = (
                        regroup(tiles, hh) * scale
                    )
        grad = jnp.concatenate([gm_ref[jq].astype(bf16) for jq in range(groups_j)], axis=1)
        glsend_ref[:, pl.ds(pl.multiple_of(b * span, span), span)] = dotf(
            rall_ref[...], grad, NT
        ).astype(bf16)
        gracc_ref[...] += dotf(left_block, grad, NN)
        return 0

    lax.fori_loop(0, chunks, backward, 0)

    def gl_copy(o):
        target = lax.rem(c + o, n_col)
        return remote(
            panel(glsend_ref, target), gl_ref.at[c], gls_sem.at[o], glr_sem.at[c], r, target
        )

    def gr_copy(k):
        return remote(
            panel(grsend_ref, k), gr_ref.at[r], grs_sem.at[k], grr_sem.at[r],
            own_row, own_col + k,
        )

    for o in range(1, n_col):
        gl_copy(o).start()
    grsend_ref[...] = gracc_ref[...].astype(bf16)
    gl_ref[c] = panel(glsend_ref, c)[...]
    for k in range(n_row):
        self_owner = (own_row == r) & (own_col + k == c)

        @pl.when(jnp.logical_not(self_owner))
        def _():
            gr_copy(k).start()

        @pl.when(self_owner)
        def _():
            gr_ref[r] = panel(grsend_ref, k)[...]

    for o in range(1, n_col):
        source = lax.rem(c + o, n_col)
        remote(
            w_rows(gwsend_ref, source), w1_ref.at[source], w1s_sem.at[o], w1r_sem.at[source],
            r, source,
        ).wait_recv()
    partial = w1_ref[0].astype(f32)
    for d in range(1, n_col):
        partial = partial + w1_ref[d].astype(f32)
    w2_ref[r] = partial.astype(bf16)

    def w2_copy(o):
        return remote(
            w2_ref.at[r], w2_ref.at[r], w2s_sem.at[o], w2r_sem.at[r], lax.rem(r + o, n_row), c
        )

    for o in range(1, n_row):
        w2_copy(o).start()

    for o in range(1, n_row):
        source = lax.rem(r + o, n_row)
        remote(
            w2_ref.at[source], w2_ref.at[source], w2s_sem.at[o], w2r_sem.at[source], source, c
        ).wait_recv()
    whole = w2_ref[0].astype(f32)
    for d in range(1, n_row):
        whole = whole + w2_ref[d].astype(f32)
    w_rows(w3_ref, c)[...] = (whole * (1.0 / total)).astype(bf16)

    def w3_copy(o):
        return remote(
            w_rows(w3_ref, c), w_rows(w3_ref, c), w3s_sem.at[o], w3r_sem.at[c],
            r, lax.rem(c + o, n_col),
        )

    for o in range(1, n_col):
        w3_copy(o).start()

    for o in range(1, n_col):
        source = lax.rem(c + o, n_col)
        remote(
            panel(glsend_ref, source), gl_ref.at[source], gls_sem.at[o], glr_sem.at[source],
            r, source,
        ).wait_recv()
    for k in range(n_row):
        self_target = loops_back & (r == k)

        @pl.when(jnp.logical_not(self_target))
        def _():
            remote(
                panel(grsend_ref, 0), gr_ref.at[k], grs_sem.at[k], grr_sem.at[k], k, to_col
            ).wait_recv()

    grad_left = gl_ref[0].astype(f32)
    for d in range(1, n_col):
        grad_left = grad_left + gl_ref[d].astype(f32)
    grad_right = gr_ref[0].astype(f32)
    for d in range(1, n_row):
        grad_right = grad_right + gr_ref[d].astype(f32)
    keep = (
        lax.broadcasted_iota(jnp.int32, (depth_s, width), 0) < depth_ref[...]
    ).astype(f32)
    sides = jnp.concatenate([grad_left * keep, grad_right * keep], axis=1)
    grad_norm = dot_exact(sides, proj_ref[...], NT) * gain_ref[...]
    normed = normed_ref[...]
    slope_ref[...] = inv_ref[...] * (
        grad_norm
        - dot_exact(grad_norm, averager, NN)
        - normed * dot_exact(grad_norm * normed, averager, NN)
    )

    for o in range(1, n_col):
        source = lax.rem(c + o, n_col)
        remote(
            w_rows(w3_ref, source), w_rows(w3_ref, source), w3s_sem.at[o], w3r_sem.at[source],
            r, source,
        ).wait_recv()
    gw_out_ref[...] = w3_ref[...].astype(f32)

    for o in range(1, n_col):
        left_copy(o).wait_send()
        w1_copy(o).wait_send()
        gl_copy(o).wait_send()
        w3_copy(o).wait_send()
    for o in range(1, n_row):
        w2_copy(o).wait_send()
    for k in range(n_row):
        self_target = loops_back & (r == k)
        self_owner = (own_row == r) & (own_col + k == c)

        @pl.when(jnp.logical_not(self_target))
        def _():
            right_copy(k).wait_send()

        @pl.when(jnp.logical_not(self_owner))
        def _():
            gr_copy(k).wait_send()


def body(
    homolog_trait_tensor,
    whitening_multiplier,
    lefthand_projection,
    righthand_projection,
    result_matrix,
    result_offset,
    sequence_tallies,
    position_molecule,
    upstream_adjoint,
):
    n_row = lax.axis_size("row")
    n_col = lax.axis_size("col")
    row_id = lax.axis_index("row")
    col_id = lax.axis_index("col")
    depth_s, full = homolog_trait_tensor.shape
    embed, hidden = lefthand_projection.shape
    pair_width = result_matrix.shape[1]
    local = full // embed
    total = local * n_row * n_col
    left_extent = total // n_row
    right_extent = total // n_col
    width = local * hidden
    channels = hidden * hidden
    rows = BLOCK * right_extent
    span = BLOCK * hidden

    table = position_molecule[:, None] == jnp.arange(sequence_tallies.shape[0])[None, :]
    depth = jnp.sum(jnp.where(table, sequence_tallies[None, :], 0), axis=1)
    depth_local = lax.dynamic_slice_in_dim(depth, (row_id * n_col + col_id) * local, local)
    depth_rows = lax.dynamic_slice_in_dim(depth, row_id * left_extent, left_extent)
    depth_cols = lax.dynamic_slice_in_dim(depth, col_id * right_extent, right_extent)
    depth_lanes = jnp.repeat(depth_local, hidden)[None, :]
    recip = 1.0 / (
        jnp.minimum(depth_rows[:, None], jnp.repeat(depth_cols, hidden)[None, :]).astype(f32)
        + EPS_COUNT
    )
    eye = jnp.eye(local, dtype=bf16)
    projections = jnp.concatenate(
        [jnp.kron(eye, lefthand_projection), jnp.kron(eye, righthand_projection)], axis=1
    )
    gain = jnp.tile(whitening_multiplier, local)[None, :]

    vmem = pl.BlockSpec(memory_space=pltpu.VMEM)
    dma = pltpu.SemaphoreType.DMA
    update, slope, grad_w = pl.pallas_call(
        functools.partial(kernel, n_row, n_col, hidden, embed),
        out_shape=(
            jax.ShapeDtypeStruct((left_extent * right_extent, pair_width), bf16),
            jax.ShapeDtypeStruct((depth_s, full), f32),
            jax.ShapeDtypeStruct((channels, pair_width), f32),
        ),
        in_specs=[vmem] * 8,
        out_specs=(vmem,) * 3,
        scratch_shapes=[
            pltpu.VMEM((depth_s, full), f32),
            pltpu.VMEM((depth_s, full), f32),
            pltpu.VMEM((depth_s, width), bf16),
            pltpu.VMEM((depth_s, width), bf16),
            pltpu.VMEM((depth_s, left_extent * hidden), bf16),
            pltpu.VMEM((depth_s, right_extent * hidden), bf16),
            pltpu.VMEM((right_extent * hidden // LANES, span, LANES), f32),
            pltpu.VMEM((rows, channels), bf16),
            pltpu.VMEM((rows, pair_width), f32),
            pltpu.VMEM((left_extent * right_extent, pair_width), bf16),
            pltpu.VMEM((rows, pair_width), f32),
            pltpu.VMEM((pair_width, channels), f32),
            pltpu.VMEM((channels, pair_width), bf16),
            pltpu.VMEM((n_col, channels // n_col, pair_width), bf16),
            pltpu.VMEM((n_row, channels // n_col, pair_width), bf16),
            pltpu.VMEM((channels, pair_width), bf16),
            pltpu.VMEM((rows, channels), f32),
            pltpu.VMEM((right_extent * hidden // LANES, span, LANES), f32),
            pltpu.VMEM((depth_s, left_extent * hidden), bf16),
            pltpu.VMEM((depth_s, right_extent * hidden), f32),
            pltpu.VMEM((depth_s, right_extent * hidden), bf16),
            pltpu.VMEM((n_col, depth_s, width), bf16),
            pltpu.VMEM((n_row, depth_s, width), bf16),
            dma((n_col,)), dma((n_col,)),
            dma((n_row,)), dma((n_row,)),
            dma((n_col,)), dma((n_col,)),
            dma((n_row,)), dma((n_row,)),
            dma((n_col,)), dma((n_col,)),
            dma((n_row,)), dma((n_row,)),
            dma((n_col,)), dma((n_col,)),
        ],
        compiler_params=pltpu.CompilerParams(
            collective_id=0, has_side_effects=True, vmem_limit_bytes=56 * 1024 * 1024
        ),
    )(
        homolog_trait_tensor,
        gain,
        projections,
        result_matrix,
        result_offset[None, :],
        depth_lanes,
        recip,
        upstream_adjoint.reshape(left_extent * right_extent, pair_width),
    )
    return update.reshape(left_extent, right_extent, pair_width), slope, grad_w


def solution(mesh):
    in_specs = (P(None, ("row", "col")), P(), P(), P(), P(), P(), P(), P(), P("row", "col", None))
    out_specs = (P("row", "col", None), P(None, ("row", "col")), P())
    return jax.shard_map(body, mesh=mesh, in_specs=in_specs, out_specs=out_specs, check_vma=False)
```

```python
import functools

import jax
import jax.numpy as jnp
from jax import lax
from jax.experimental import pallas as pl
from jax.experimental.pallas import tpu as pltpu
from jax.sharding import PartitionSpec as P

EPS_NORM = 1e-05
EPS_COUNT = 0.001
LANES = 128
BLOCK = 32

f32 = jnp.float32
bf16 = jnp.bfloat16


def dotf(a, b, dims):
    return lax.dot_general(a, b, (dims, ((), ())), preferred_element_type=f32)


def dot_exact(a, b, dims):
    first = a.astype(bf16)
    rest = a - first.astype(f32)
    second = rest.astype(bf16)
    third = (rest - second.astype(f32)).astype(bf16)
    return dotf(third, b, dims) + dotf(second, b, dims) + dotf(first, b, dims)


NN = ((1,), (0,))
NT = ((1,), (1,))
TN = ((0,), (0,))


def kernel(
    n_row, n_col, hidden, embed,
    x_ref, gain_ref, proj_ref, w_ref, offset_ref, depth_ref, recip_ref, adj_ref,
    upd_ref, slope_ref, gw_out_ref,
    normed_ref, inv_ref, lsend_ref, rsend_ref, lall_ref, rall_ref, prod_ref, flat_ref,
    adjf_ref, adjt_ref, updf_ref, gacc_ref, gwsend_ref, w1_ref, w2send_ref, w2_ref, w4_ref,
    go_ref, gm_ref, glsend_ref, glp_ref, glsum_ref, gl_ref,
    gracc_ref, grsend_ref, gr_ref, grsum_ref, grfin_ref,
    ls_sem, lf_sem, lr_sem, rs_sem, rr_sem, gps_sem, gpr_sem, gls_sem, glr_sem,
    grs_sem, grr_sem, hop_sem, w1s_sem, w1r_sem, w2s_sem, w2r_sem, w3s_sem, w3r_sem,
    w4s_sem, w4r_sem,
):
    r = lax.axis_index("row")
    c = lax.axis_index("col")
    group = n_col // n_row
    depth_s = x_ref.shape[0]
    width = lsend_ref.shape[1]
    per_vreg = LANES // hidden
    left_extent = recip_ref.shape[0]
    right_extent = recip_ref.shape[1] // hidden
    chunks = left_extent // BLOCK
    channels = hidden * hidden
    total = n_row * n_col * (x_ref.shape[1] // embed)

    to_col = r * group + c // n_row
    to_slot = lax.rem(c, n_row)
    own_row = c // group
    own_col = lax.rem(c, group) * n_row
    fixed = (to_col == c) & (to_slot == r)
    half = n_col // 2
    pair, side = c // 2, lax.rem(c, 2)
    partner = c + 1 - 2 * side

    barrier = pltpu.get_barrier_semaphore()

    def greet(row, col):
        pl.semaphore_signal(
            barrier, inc=1, device_id=(row, col), device_id_type=pl.DeviceIdType.MESH
        )

    for o in range(1, n_col):
        greet(r, lax.rem(c + o, n_col))
    for o in range(1, n_row):
        greet(lax.rem(r + o, n_row), c)

    @pl.when(jnp.logical_not(fixed))
    def _():
        greet(to_slot, to_col)
        greet(own_row, own_col + r)

    def remote(src, dst, send_sem, recv_sem, row, col):
        return pltpu.make_async_remote_copy(
            src_ref=src, dst_ref=dst, send_sem=send_sem, recv_sem=recv_sem,
            device_id=(row, col), device_id_type=pl.DeviceIdType.MESH,
        )

    full = x_ref.shape[1]
    same = (
        lax.broadcasted_iota(jnp.int32, (full, full), 0) // embed
        == lax.broadcasted_iota(jnp.int32, (full, full), 1) // embed
    )
    averager = jnp.where(same, 1.0 / embed, 0.0).astype(bf16)
    x = x_ref[...]
    centred = x.astype(f32) - dotf(x, averager, NN)
    inv = lax.rsqrt(dot_exact(centred * centred, averager, NN) + EPS_NORM)
    normed = centred * inv
    normed_ref[...] = normed
    inv_ref[...] = inv
    gain = gain_ref[...]
    keep = (
        lax.broadcasted_iota(jnp.int32, (depth_s, width), 0) < depth_ref[...]
    ).astype(f32)
    both = dot_exact(normed * gain, proj_ref[...], NN)
    left = (both[:, :width] * keep).astype(bf16)
    right = (both[:, width:] * keep).astype(bf16)
    rsend_ref[...] = right
    lsend_ref[...] = left

    def panel(ref, index):
        return ref.at[:, pl.ds(pl.multiple_of(index * width, LANES), width)]

    pl.semaphore_wait(
        barrier, n_col - 1 + n_row - 1 + 2 - 2 * fixed.astype(jnp.int32)
    )

    def same_side(o):
        return lax.rem(pair + o, half) * 2 + side

    def right_hop():
        return remote(
            rsend_ref, panel(rall_ref, to_slot), hop_sem.at[0], rr_sem.at[to_slot],
            to_slot, to_col,
        )

    def right_copy(o):
        return remote(
            panel(rall_ref, r), panel(rall_ref, r), rs_sem.at[o], rr_sem.at[r],
            lax.rem(r + o, n_row), c,
        )

    def left_copy(o):
        target = partner if o == 0 else same_side(o)
        return remote(lsend_ref, panel(lall_ref, c), ls_sem.at[o], lr_sem.at[c], r, target)

    def left_relay(o):
        source = same_side(half - o)
        return remote(
            panel(lall_ref, source), panel(lall_ref, source), lf_sem.at[o], lr_sem.at[source],
            r, partner,
        )

    def left_arrival(source):
        remote(
            lsend_ref, panel(lall_ref, source), ls_sem.at[0], lr_sem.at[source], r, partner
        ).wait_recv()

    @pl.when(jnp.logical_not(fixed))
    def _():
        right_hop().start()

    @pl.when(fixed)
    def _():
        panel(rall_ref, r)[...] = rsend_ref[...]

    for o in range(half):
        left_copy(o).start()

    panel(lall_ref, c)[...] = left

    rows = BLOCK * right_extent
    for b in range(chunks):
        adjf_ref[...] = adj_ref[b * rows : (b + 1) * rows, :].astype(f32)
        for j in range(right_extent):
            adjt_ref[b * rows + j * BLOCK : b * rows + (j + 1) * BLOCK, :] = adjf_ref[
                pl.ds(j, BLOCK, stride=right_extent), :
            ].astype(bf16)

    def right_arrival(slot):
        remote(
            rsend_ref, panel(rall_ref, slot), hop_sem.at[0], rr_sem.at[slot],
            to_slot, to_col,
        ).wait_recv()

    @pl.when(jnp.logical_not(fixed))
    def _():
        right_arrival(r)

    for o in range(1, n_row):
        right_copy(o).start()
    for o in range(1, half):
        left_arrival(same_side(half - o))
        left_relay(o).start()
    for o in range(1, n_row):
        right_arrival(lax.rem(r + o, n_row))
    for o in range(half):
        left_arrival(lax.rem(pair + o, half) * 2 + 1 - side)

    lane_part = lax.broadcasted_iota(jnp.int32, (BLOCK, LANES), 1) // hidden
    groups_j = right_extent // per_vreg
    groups_h = hidden // per_vreg

    def regroup(tiles, own):
        merged = None
        for t in range(per_vreg):
            shift = ((t - own) * hidden) % LANES
            moved = pltpu.roll(tiles[t], shift, 1) if shift else tiles[t]
            merged = moved if merged is None else jnp.where(lane_part == t, moved, merged)
        return merged

    span = BLOCK * hidden
    gacc_ref[...] = jnp.zeros_like(gacc_ref)

    def forward(b, _):
        start = pl.multiple_of(b * rows, rows)
        recip = recip_ref[pl.ds(pl.multiple_of(b * BLOCK, BLOCK), BLOCK), :]
        left_block = lall_ref[:, pl.ds(pl.multiple_of(b * span, span), span)]
        product = dotf(left_block, rall_ref[...], TN)
        for jq in range(groups_j):
            prod_ref[jq] = product[:, jq * LANES : (jq + 1) * LANES]
        for hq in range(groups_h):
            for jq in range(groups_j):
                scale = recip[:, jq * LANES : (jq + 1) * LANES]
                tiles = [
                    prod_ref[jq, pl.ds(hq * per_vreg + t, BLOCK, stride=hidden), :] * scale
                    for t in range(per_vreg)
                ]
                for jj in range(per_vreg):
                    j = jq * per_vreg + jj
                    flat_ref[
                        j * BLOCK : (j + 1) * BLOCK, hq * LANES : (hq + 1) * LANES
                    ] = regroup(tiles, jj).astype(bf16)
        flat = flat_ref[...]
        incoming = adjt_ref[pl.ds(start, rows), :]
        gacc_ref[...] += dotf(incoming, flat, TN)
        update = dotf(flat, w_ref[...], NN) + offset_ref[...]
        for j in range(right_extent):
            updf_ref[pl.ds(j, BLOCK, stride=right_extent), :] = update[
                j * BLOCK : (j + 1) * BLOCK, :
            ]
        upd_ref[pl.ds(start, rows), :] = updf_ref[...].astype(bf16)
        return 0

    lax.fori_loop(0, chunks, forward, 0)

    part = channels // n_row
    piece = part // n_col
    gwsend_ref[...] = gacc_ref[...].T.reshape(n_row, part, gacc_ref.shape[0]).astype(bf16)

    def w1_copy(o):
        target = lax.rem(r + o, n_row)
        return remote(
            gwsend_ref.at[target], w1_ref.at[r], w1s_sem.at[o], w1r_sem.at[r], target, c
        )

    for o in range(1, n_row):
        w1_copy(o).start()
    w1_ref[r] = gwsend_ref[r]

    gracc_ref[...] = jnp.zeros_like(gracc_ref)

    def backward(b, _):
        start = pl.multiple_of(b * rows, rows)
        recip = recip_ref[pl.ds(pl.multiple_of(b * BLOCK, BLOCK), BLOCK), :]
        left_block = lall_ref[:, pl.ds(pl.multiple_of(b * span, span), span)]
        go_ref[...] = dotf(adjt_ref[pl.ds(start, rows), :], w_ref[...], NT)
        for hq in range(groups_h):
            for jq in range(groups_j):
                scale = recip[:, jq * LANES : (jq + 1) * LANES]
                tiles = [
                    go_ref[
                        (jq * per_vreg + t) * BLOCK : (jq * per_vreg + t + 1) * BLOCK,
                        hq * LANES : (hq + 1) * LANES,
                    ]
                    for t in range(per_vreg)
                ]
                for hh in range(per_vreg):
                    gm_ref[jq, pl.ds(hq * per_vreg + hh, BLOCK, stride=hidden), :] = (
                        regroup(tiles, hh) * scale
                    )
        grad = jnp.concatenate([gm_ref[jq].astype(bf16) for jq in range(groups_j)], axis=1)
        glsend_ref[:, pl.ds(pl.multiple_of(b * span, span), span)] = dotf(
            rall_ref[...], grad, NT
        ).astype(bf16)
        gracc_ref[...] += dotf(left_block, grad, NN)
        return 0

    lax.fori_loop(0, chunks, backward, 0)

    def gp_copy(o):
        q = lax.rem(pair + o, half)
        return remote(
            panel(glsend_ref, q * 2 + 1 - side), glp_ref.at[q], gps_sem.at[o], gpr_sem.at[q],
            r, partner,
        )

    def gl_copy(o):
        q = lax.rem(pair + o, half)
        return remote(
            glsum_ref.at[q], gl_ref.at[pair], gls_sem.at[o], glr_sem.at[pair], r, q * 2 + side
        )

    def gr_copy(o):
        target = lax.rem(r + o, n_row)
        return remote(
            panel(grsend_ref, target), gr_ref.at[r], grs_sem.at[o], grr_sem.at[r], target, c
        )

    def gr_hop():
        return remote(
            grsum_ref, grfin_ref, hop_sem.at[1], hop_sem.at[2], own_row, own_col + r
        )

    def w2_copy(o):
        target = lax.rem(c + o, n_col)
        return remote(
            w2send_ref.at[target], w2_ref.at[c], w2s_sem.at[o], w2r_sem.at[c], r, target
        )

    def w3_copy(o):
        return remote(
            w4_ref.at[r, c], w4_ref.at[r, c], w3s_sem.at[o], w3r_sem.at[c],
            r, lax.rem(c + o, n_col),
        )

    def w4_copy(o):
        return remote(
            w4_ref.at[r], w4_ref.at[r], w4s_sem.at[o], w4r_sem.at[r], lax.rem(r + o, n_row), c
        )

    for step in range(1, half + 1):
        gp_copy(step % half).start()
    grsend_ref[...] = gracc_ref[...].astype(bf16)
    for o in range(1, n_row):
        gr_copy(o).start()
    gr_ref[r] = panel(grsend_ref, r)[...]

    for o in range(1, n_row):
        source = lax.rem(r + o, n_row)
        remote(
            gwsend_ref.at[source], w1_ref.at[source], w1s_sem.at[o], w1r_sem.at[source],
            source, c,
        ).wait_recv()
    partial = w1_ref[0].astype(f32)
    for d in range(1, n_row):
        partial = partial + w1_ref[d].astype(f32)
    w2send_ref[...] = partial.reshape(n_col, piece, partial.shape[1]).astype(bf16)
    w2_ref[c] = w2send_ref[c]
    for o in range(1, n_col):
        w2_copy(o).start()

    for step in range(1, half + 1):
        o = step % half
        q = lax.rem(pair + o, half)
        remote(
            panel(glsend_ref, 0), glp_ref.at[q], gps_sem.at[o], gpr_sem.at[q], r, partner
        ).wait_recv()
        joint = panel(glsend_ref, q * 2 + side)[...].astype(f32) + glp_ref[q].astype(f32)
        if o:
            glsum_ref[q] = joint.astype(bf16)
            gl_copy(o).start()
        else:
            gl_ref[pair] = joint.astype(bf16)

    for o in range(1, n_row):
        source = lax.rem(r + o, n_row)
        remote(
            panel(grsend_ref, source), gr_ref.at[source], grs_sem.at[o], grr_sem.at[source],
            source, c,
        ).wait_recv()
    grad_right = gr_ref[0].astype(f32)
    for d in range(1, n_row):
        grad_right = grad_right + gr_ref[d].astype(f32)
    grsum_ref[...] = grad_right.astype(bf16)

    @pl.when(jnp.logical_not(fixed))
    def _():
        gr_hop().start()

    @pl.when(fixed)
    def _():
        grfin_ref[...] = grsum_ref[...]

    for o in range(1, n_col):
        source = lax.rem(c + o, n_col)
        remote(
            w2send_ref.at[source], w2_ref.at[source], w2s_sem.at[o], w2r_sem.at[source],
            r, source,
        ).wait_recv()
    whole = w2_ref[0].astype(f32)
    for d in range(1, n_col):
        whole = whole + w2_ref[d].astype(f32)
    w4_ref[r, c] = (whole * (1.0 / total)).astype(bf16)
    for o in range(1, n_col):
        w3_copy(o).start()

    for o in range(1, half):
        source = lax.rem(pair + o, half)
        remote(
            glsum_ref.at[source], gl_ref.at[source], gls_sem.at[o], glr_sem.at[source],
            r, source * 2 + side,
        ).wait_recv()

    @pl.when(jnp.logical_not(fixed))
    def _():
        gr_hop().wait_recv()

    for o in range(1, n_col):
        source = lax.rem(c + o, n_col)
        remote(
            w4_ref.at[r, source], w4_ref.at[r, source], w3s_sem.at[o], w3r_sem.at[source],
            r, source,
        ).wait_recv()
    for o in range(1, n_row):
        w4_copy(o).start()

    grad_left = gl_ref[0].astype(f32)
    for d in range(1, half):
        grad_left = grad_left + gl_ref[d].astype(f32)
    grad_right = grfin_ref[...].astype(f32)
    keep = (
        lax.broadcasted_iota(jnp.int32, (depth_s, width), 0) < depth_ref[...]
    ).astype(f32)
    sides = jnp.concatenate([grad_left * keep, grad_right * keep], axis=1)
    grad_norm = dot_exact(sides, proj_ref[...], NT) * gain_ref[...]
    normed = normed_ref[...]
    slope_ref[...] = inv_ref[...] * (
        grad_norm
        - dot_exact(grad_norm, averager, NN)
        - normed * dot_exact(grad_norm * normed, averager, NN)
    )

    for o in range(1, n_row):
        source = lax.rem(r + o, n_row)
        remote(
            w4_ref.at[source], w4_ref.at[source], w4s_sem.at[o], w4r_sem.at[source], source, c
        ).wait_recv()
    gw_out_ref[...] = w4_ref[...].astype(f32).reshape(gw_out_ref.shape)

    for o in range(half):
        left_copy(o).wait_send()
        gp_copy(o).wait_send()
    for o in range(1, half):
        left_relay(o).wait_send()
        gl_copy(o).wait_send()
    for o in range(1, n_col):
        w2_copy(o).wait_send()
        w3_copy(o).wait_send()
    for o in range(1, n_row):
        right_copy(o).wait_send()
        gr_copy(o).wait_send()
        w1_copy(o).wait_send()
        w4_copy(o).wait_send()

    @pl.when(jnp.logical_not(fixed))
    def _():
        right_hop().wait_send()
        gr_hop().wait_send()


def body(
    homolog_trait_tensor,
    whitening_multiplier,
    lefthand_projection,
    righthand_projection,
    result_matrix,
    result_offset,
    sequence_tallies,
    position_molecule,
    upstream_adjoint,
):
    n_row = lax.axis_size("row")
    n_col = lax.axis_size("col")
    row_id = lax.axis_index("row")
    col_id = lax.axis_index("col")
    depth_s, full = homolog_trait_tensor.shape
    embed, hidden = lefthand_projection.shape
    pair_width = result_matrix.shape[1]
    local = full // embed
    total = local * n_row * n_col
    left_extent = total // n_row
    right_extent = total // n_col
    width = local * hidden
    channels = hidden * hidden
    rows = BLOCK * right_extent
    span = BLOCK * hidden
    half = n_col // 2
    piece = channels // (n_row * n_col)

    table = position_molecule[:, None] == jnp.arange(sequence_tallies.shape[0])[None, :]
    depth = jnp.sum(jnp.where(table, sequence_tallies[None, :], 0), axis=1)
    depth_local = lax.dynamic_slice_in_dim(depth, (row_id * n_col + col_id) * local, local)
    depth_rows = lax.dynamic_slice_in_dim(depth, row_id * left_extent, left_extent)
    depth_cols = lax.dynamic_slice_in_dim(depth, col_id * right_extent, right_extent)
    depth_lanes = jnp.repeat(depth_local, hidden)[None, :]
    recip = 1.0 / (
        jnp.minimum(depth_rows[:, None], jnp.repeat(depth_cols, hidden)[None, :]).astype(f32)
        + EPS_COUNT
    )
    eye = jnp.eye(local, dtype=bf16)
    projections = jnp.concatenate(
        [jnp.kron(eye, lefthand_projection), jnp.kron(eye, righthand_projection)], axis=1
    )
    gain = jnp.tile(whitening_multiplier, local)[None, :]

    vmem = pl.BlockSpec(memory_space=pltpu.VMEM)
    dma = pltpu.SemaphoreType.DMA
    update, slope, grad_w = pl.pallas_call(
        functools.partial(kernel, n_row, n_col, hidden, embed),
        out_shape=(
            jax.ShapeDtypeStruct((left_extent * right_extent, pair_width), bf16),
            jax.ShapeDtypeStruct((depth_s, full), f32),
            jax.ShapeDtypeStruct((channels, pair_width), f32),
        ),
        in_specs=[vmem] * 8,
        out_specs=(vmem,) * 3,
        scratch_shapes=[
            pltpu.VMEM((depth_s, full), f32),
            pltpu.VMEM((depth_s, full), f32),
            pltpu.VMEM((depth_s, width), bf16),
            pltpu.VMEM((depth_s, width), bf16),
            pltpu.VMEM((depth_s, left_extent * hidden), bf16),
            pltpu.VMEM((depth_s, right_extent * hidden), bf16),
            pltpu.VMEM((right_extent * hidden // LANES, span, LANES), f32),
            pltpu.VMEM((rows, channels), bf16),
            pltpu.VMEM((rows, pair_width), f32),
            pltpu.VMEM((left_extent * right_extent, pair_width), bf16),
            pltpu.VMEM((rows, pair_width), f32),
            pltpu.VMEM((pair_width, channels), f32),
            pltpu.VMEM((n_row, channels // n_row, pair_width), bf16),
            pltpu.VMEM((n_row, channels // n_row, pair_width), bf16),
            pltpu.VMEM((n_col, piece, pair_width), bf16),
            pltpu.VMEM((n_col, piece, pair_width), bf16),
            pltpu.VMEM((n_row, n_col, piece, pair_width), bf16),
            pltpu.VMEM((rows, channels), f32),
            pltpu.VMEM((right_extent * hidden // LANES, span, LANES), f32),
            pltpu.VMEM((depth_s, left_extent * hidden), bf16),
            pltpu.VMEM((half, depth_s, width), bf16),
            pltpu.VMEM((half, depth_s, width), bf16),
            pltpu.VMEM((half, depth_s, width), bf16),
            pltpu.VMEM((depth_s, right_extent * hidden), f32),
            pltpu.VMEM((depth_s, right_extent * hidden), bf16),
            pltpu.VMEM((n_row, depth_s, width), bf16),
            pltpu.VMEM((depth_s, width), bf16),
            pltpu.VMEM((depth_s, width), bf16),
            dma((half,)), dma((half,)), dma((n_col,)),
            dma((n_row,)), dma((n_row,)),
            dma((half,)), dma((half,)), dma((half,)), dma((half,)),
            dma((n_row,)), dma((n_row,)), dma((3,)),
            dma((n_row,)), dma((n_row,)), dma((n_col,)), dma((n_col,)),
            dma((n_col,)), dma((n_col,)), dma((n_row,)), dma((n_row,)),
        ],
        compiler_params=pltpu.CompilerParams(
            collective_id=0, has_side_effects=True, vmem_limit_bytes=56 * 1024 * 1024
        ),
    )(
        homolog_trait_tensor,
        gain,
        projections,
        result_matrix,
        result_offset[None, :],
        depth_lanes,
        recip,
        upstream_adjoint.reshape(left_extent * right_extent, pair_width),
    )
    return update.reshape(left_extent, right_extent, pair_width), slope, grad_w


def solution(mesh):
    in_specs = (P(None, ("row", "col")), P(), P(), P(), P(), P(), P(), P(), P("row", "col", None))
    out_specs = (P("row", "col", None), P(None, ("row", "col")), P())
    return jax.shard_map(body, mesh=mesh, in_specs=in_specs, out_specs=out_specs, check_vma=False)
```

```python
import functools

import jax
import jax.numpy as jnp
from jax import lax
from jax.experimental import pallas as pl
from jax.experimental.pallas import tpu as pltpu
from jax.sharding import PartitionSpec as P

EPS_NORM = 1e-05
EPS_COUNT = 0.001
LANES = 128
BLOCK = 32

f32 = jnp.float32
bf16 = jnp.bfloat16


def dotf(a, b, dims):
    return lax.dot_general(a, b, (dims, ((), ())), preferred_element_type=f32)


def dot_exact(a, b, dims):
    first = a.astype(bf16)
    rest = a - first.astype(f32)
    second = rest.astype(bf16)
    third = (rest - second.astype(f32)).astype(bf16)
    return dotf(third, b, dims) + dotf(second, b, dims) + dotf(first, b, dims)


NN = ((1,), (0,))
NT = ((1,), (1,))
TN = ((0,), (0,))


def kernel(
    n_row, n_col, hidden, embed,
    x_ref, gain_ref, proj_ref, w_ref, offset_ref, tallies_ref, position_ref, adj_ref,
    upd_ref, slope_ref, gw_out_ref,
    normed_ref, inv_ref, lsend_ref, rsend_ref, lall_ref, rall_ref, prod_ref, flat_ref,
    adjf_ref, adjt_ref, updf_ref, gacc_ref, gwsend_ref, w1_ref, w2send_ref, w2_ref, w4_ref,
    go_ref, gm_ref, glsend_ref, glp_ref, glsum_ref, gl_ref,
    gracc_ref, grsend_ref, gr_ref, grsum_ref, grfin_ref,
    ls_sem, lf_sem, lr_sem, rs_sem, rr_sem, gps_sem, gpr_sem, gls_sem, glr_sem,
    grs_sem, grr_sem, hop_sem, w1s_sem, w1r_sem, w2s_sem, w2r_sem, w3s_sem, w3r_sem,
    w4s_sem, w4r_sem, recip_ref, keep_ref,
):
    r = lax.axis_index("row")
    c = lax.axis_index("col")
    group = n_col // n_row
    depth_s = x_ref.shape[0]
    width = lsend_ref.shape[1]
    per_vreg = LANES // hidden
    left_extent = recip_ref.shape[0]
    right_extent = recip_ref.shape[1] // hidden
    chunks = left_extent // BLOCK
    channels = hidden * hidden
    total = n_row * n_col * (x_ref.shape[1] // embed)

    to_col = r * group + c // n_row
    to_slot = lax.rem(c, n_row)
    own_row = c // group
    own_col = lax.rem(c, group) * n_row
    fixed = (to_col == c) & (to_slot == r)
    half = n_col // 2
    pair, side = c // 2, lax.rem(c, 2)
    partner = c + 1 - 2 * side

    barrier = pltpu.get_barrier_semaphore()

    def greet(row, col):
        pl.semaphore_signal(
            barrier, inc=1, device_id=(row, col), device_id_type=pl.DeviceIdType.MESH
        )

    for o in range(1, n_col):
        greet(r, lax.rem(c + o, n_col))
    for o in range(1, n_row):
        greet(lax.rem(r + o, n_row), c)

    @pl.when(jnp.logical_not(fixed))
    def _():
        greet(to_slot, to_col)
        greet(own_row, own_col + r)

    def remote(src, dst, send_sem, recv_sem, row, col):
        return pltpu.make_async_remote_copy(
            src_ref=src, dst_ref=dst, send_sem=send_sem, recv_sem=recv_sem,
            device_id=(row, col), device_id_type=pl.DeviceIdType.MESH,
        )

    full = x_ref.shape[1]
    same = (
        lax.broadcasted_iota(jnp.int32, (full, full), 0) // embed
        == lax.broadcasted_iota(jnp.int32, (full, full), 1) // embed
    )
    averager = jnp.where(same, 1.0 / embed, 0.0).astype(bf16)
    x = x_ref[...]
    centred = x.astype(f32) - dotf(x, averager, NN)
    inv = lax.rsqrt(dot_exact(centred * centred, averager, NN) + EPS_NORM)
    normed = centred * inv
    normed_ref[...] = normed
    inv_ref[...] = inv
    gain = jnp.concatenate([gain_ref[...]] * (full // embed), axis=1)

    def spread(shape, axis, each, first, count):
        place = lax.broadcasted_iota(jnp.int32, shape, axis) // each
        depths = jnp.zeros(shape, jnp.int32)
        for t in range(count):
            depths = jnp.where(place == t, tallies_ref[position_ref[first + t]], depths)
        return depths

    local = full // embed
    keep = (
        lax.broadcasted_iota(jnp.int32, (depth_s, width), 0)
        < spread((1, width), 1, hidden, (r * n_col + c) * local, local)
    ).astype(f32)
    keep_ref[...] = keep
    both = dot_exact(normed * gain, proj_ref[...], NN)
    left = (both[:, :width] * keep).astype(bf16)
    right = (both[:, width:] * keep).astype(bf16)
    rsend_ref[...] = right
    lsend_ref[...] = left

    def panel(ref, index):
        return ref.at[:, pl.ds(pl.multiple_of(index * width, LANES), width)]

    pl.semaphore_wait(
        barrier, n_col - 1 + n_row - 1 + 2 - 2 * fixed.astype(jnp.int32)
    )

    def same_side(o):
        return lax.rem(pair + o, half) * 2 + side

    def right_hop():
        return remote(
            rsend_ref, panel(rall_ref, to_slot), hop_sem.at[0], rr_sem.at[to_slot],
            to_slot, to_col,
        )

    def right_copy(o):
        return remote(
            panel(rall_ref, r), panel(rall_ref, r), rs_sem.at[o], rr_sem.at[r],
            lax.rem(r + o, n_row), c,
        )

    def left_copy(o):
        target = partner if o == 0 else same_side(o)
        return remote(lsend_ref, panel(lall_ref, c), ls_sem.at[o], lr_sem.at[c], r, target)

    def left_relay(o):
        source = same_side(half - o)
        return remote(
            panel(lall_ref, source), panel(lall_ref, source), lf_sem.at[o], lr_sem.at[source],
            r, partner,
        )

    def left_arrival(source):
        remote(
            lsend_ref, panel(lall_ref, source), ls_sem.at[0], lr_sem.at[source], r, partner
        ).wait_recv()

    @pl.when(jnp.logical_not(fixed))
    def _():
        right_hop().start()

    @pl.when(fixed)
    def _():
        panel(rall_ref, r)[...] = rsend_ref[...]

    for o in range(half):
        left_copy(o).start()

    panel(lall_ref, c)[...] = left

    rows = BLOCK * right_extent
    over_cols = spread(
        (1, recip_ref.shape[1]), 1, hidden, c * right_extent, right_extent
    )
    for b in range(chunks):
        over_rows = spread((BLOCK, 1), 0, 1, r * left_extent + b * BLOCK, BLOCK)
        counts = jnp.minimum(over_rows, over_cols).astype(f32) + EPS_COUNT
        recip_ref[b * BLOCK : (b + 1) * BLOCK, :] = 1.0 / counts
        adjf_ref[...] = adj_ref[b * rows : (b + 1) * rows, :].astype(f32)
        for j in range(right_extent):
            adjt_ref[b * rows + j * BLOCK : b * rows + (j + 1) * BLOCK, :] = adjf_ref[
                pl.ds(j, BLOCK, stride=right_extent), :
            ].astype(bf16)

    def right_arrival(slot):
        remote(
            rsend_ref, panel(rall_ref, slot), hop_sem.at[0], rr_sem.at[slot],
            to_slot, to_col,
        ).wait_recv()

    @pl.when(jnp.logical_not(fixed))
    def _():
        right_arrival(r)

    for o in range(1, n_row):
        right_copy(o).start()
    for o in range(1, half):
        left_arrival(same_side(half - o))
        left_relay(o).start()
    for o in range(1, n_row):
        right_arrival(lax.rem(r + o, n_row))
    for o in range(half):
        left_arrival(lax.rem(pair + o, half) * 2 + 1 - side)

    lane_part = lax.broadcasted_iota(jnp.int32, (BLOCK, LANES), 1) // hidden
    groups_j = right_extent // per_vreg
    groups_h = hidden // per_vreg

    def regroup(tiles, own):
        merged = None
        for t in range(per_vreg):
            shift = ((t - own) * hidden) % LANES
            moved = pltpu.roll(tiles[t], shift, 1) if shift else tiles[t]
            merged = moved if merged is None else jnp.where(lane_part == t, moved, merged)
        return merged

    span = BLOCK * hidden
    gacc_ref[...] = jnp.zeros_like(gacc_ref)

    def forward(b, _):
        start = pl.multiple_of(b * rows, rows)
        recip = recip_ref[pl.ds(pl.multiple_of(b * BLOCK, BLOCK), BLOCK), :]
        left_block = lall_ref[:, pl.ds(pl.multiple_of(b * span, span), span)]
        product = dotf(left_block, rall_ref[...], TN)
        for jq in range(groups_j):
            prod_ref[jq] = product[:, jq * LANES : (jq + 1) * LANES]
        for hq in range(groups_h):
            for jq in range(groups_j):
                scale = recip[:, jq * LANES : (jq + 1) * LANES]
                tiles = [
                    prod_ref[jq, pl.ds(hq * per_vreg + t, BLOCK, stride=hidden), :] * scale
                    for t in range(per_vreg)
                ]
                for jj in range(per_vreg):
                    j = jq * per_vreg + jj
                    flat_ref[
                        j * BLOCK : (j + 1) * BLOCK, hq * LANES : (hq + 1) * LANES
                    ] = regroup(tiles, jj).astype(bf16)
        flat = flat_ref[...]
        incoming = adjt_ref[pl.ds(start, rows), :]
        gacc_ref[...] += dotf(incoming, flat, TN)
        update = dotf(flat, w_ref[...], NN) + offset_ref[...]
        for j in range(right_extent):
            updf_ref[pl.ds(j, BLOCK, stride=right_extent), :] = update[
                j * BLOCK : (j + 1) * BLOCK, :
            ]
        upd_ref[pl.ds(start, rows), :] = updf_ref[...].astype(bf16)
        return 0

    lax.fori_loop(0, chunks, forward, 0)

    part = channels // n_row
    piece = part // n_col
    gwsend_ref[...] = gacc_ref[...].T.reshape(n_row, part, gacc_ref.shape[0]).astype(bf16)

    def w1_copy(o):
        target = lax.rem(r + o, n_row)
        return remote(
            gwsend_ref.at[target], w1_ref.at[r], w1s_sem.at[o], w1r_sem.at[r], target, c
        )

    for o in range(1, n_row):
        w1_copy(o).start()
    w1_ref[r] = gwsend_ref[r]

    gracc_ref[...] = jnp.zeros_like(gracc_ref)

    def backward(b, _):
        start = pl.multiple_of(b * rows, rows)
        recip = recip_ref[pl.ds(pl.multiple_of(b * BLOCK, BLOCK), BLOCK), :]
        left_block = lall_ref[:, pl.ds(pl.multiple_of(b * span, span), span)]
        go_ref[...] = dotf(adjt_ref[pl.ds(start, rows), :], w_ref[...], NT)
        for hq in range(groups_h):
            for jq in range(groups_j):
                scale = recip[:, jq * LANES : (jq + 1) * LANES]
                tiles = [
                    go_ref[
                        (jq * per_vreg + t) * BLOCK : (jq * per_vreg + t + 1) * BLOCK,
                        hq * LANES : (hq + 1) * LANES,
                    ]
                    for t in range(per_vreg)
                ]
                for hh in range(per_vreg):
                    gm_ref[jq, pl.ds(hq * per_vreg + hh, BLOCK, stride=hidden), :] = (
                        regroup(tiles, hh) * scale
                    )
        grad = jnp.concatenate([gm_ref[jq].astype(bf16) for jq in range(groups_j)], axis=1)
        glsend_ref[:, pl.ds(pl.multiple_of(b * span, span), span)] = dotf(
            rall_ref[...], grad, NT
        ).astype(bf16)
        gracc_ref[...] += dotf(left_block, grad, NN)
        return 0

    lax.fori_loop(0, chunks, backward, 0)

    def gp_copy(o):
        q = lax.rem(pair + o, half)
        return remote(
            panel(glsend_ref, q * 2 + 1 - side), glp_ref.at[q], gps_sem.at[o], gpr_sem.at[q],
            r, partner,
        )

    def gl_copy(o):
        q = lax.rem(pair + o, half)
        return remote(
            glsum_ref.at[q], gl_ref.at[pair], gls_sem.at[o], glr_sem.at[pair], r, q * 2 + side
        )

    def gr_copy(o):
        target = lax.rem(r + o, n_row)
        return remote(
            panel(grsend_ref, target), gr_ref.at[r], grs_sem.at[o], grr_sem.at[r], target, c
        )

    def gr_hop():
        return remote(
            grsum_ref, grfin_ref, hop_sem.at[1], hop_sem.at[2], own_row, own_col + r
        )

    def w2_copy(o):
        target = lax.rem(c + o, n_col)
        return remote(
            w2send_ref.at[target], w2_ref.at[c], w2s_sem.at[o], w2r_sem.at[c], r, target
        )

    def w3_copy(o):
        return remote(
            w4_ref.at[r, c], w4_ref.at[r, c], w3s_sem.at[o], w3r_sem.at[c],
            r, lax.rem(c + o, n_col),
        )

    def w4_copy(o):
        return remote(
            w4_ref.at[r], w4_ref.at[r], w4s_sem.at[o], w4r_sem.at[r], lax.rem(r + o, n_row), c
        )

    for step in range(1, half + 1):
        gp_copy(step % half).start()
    grsend_ref[...] = gracc_ref[...].astype(bf16)
    for o in range(1, n_row):
        gr_copy(o).start()
    gr_ref[r] = panel(grsend_ref, r)[...]

    for o in range(1, n_row):
        source = lax.rem(r + o, n_row)
        remote(
            gwsend_ref.at[source], w1_ref.at[source], w1s_sem.at[o], w1r_sem.at[source],
            source, c,
        ).wait_recv()
    partial = w1_ref[0].astype(f32)
    for d in range(1, n_row):
        partial = partial + w1_ref[d].astype(f32)
    w2send_ref[...] = partial.reshape(n_col, piece, partial.shape[1]).astype(bf16)
    w2_ref[c] = w2send_ref[c]
    for o in range(1, n_col):
        w2_copy(o).start()

    for step in range(1, half + 1):
        o = step % half
        q = lax.rem(pair + o, half)
        remote(
            panel(glsend_ref, 0), glp_ref.at[q], gps_sem.at[o], gpr_sem.at[q], r, partner
        ).wait_recv()
        joint = panel(glsend_ref, q * 2 + side)[...].astype(f32) + glp_ref[q].astype(f32)
        if o:
            glsum_ref[q] = joint.astype(bf16)
            gl_copy(o).start()
        else:
            gl_ref[pair] = joint.astype(bf16)

    for o in range(1, n_row):
        source = lax.rem(r + o, n_row)
        remote(
            panel(grsend_ref, source), gr_ref.at[source], grs_sem.at[o], grr_sem.at[source],
            source, c,
        ).wait_recv()
    grad_right = gr_ref[0].astype(f32)
    for d in range(1, n_row):
        grad_right = grad_right + gr_ref[d].astype(f32)
    grsum_ref[...] = grad_right.astype(bf16)

    @pl.when(jnp.logical_not(fixed))
    def _():
        gr_hop().start()

    @pl.when(fixed)
    def _():
        grfin_ref[...] = grsum_ref[...]

    for o in range(1, n_col):
        source = lax.rem(c + o, n_col)
        remote(
            w2send_ref.at[source], w2_ref.at[source], w2s_sem.at[o], w2r_sem.at[source],
            r, source,
        ).wait_recv()
    whole = w2_ref[0].astype(f32)
    for d in range(1, n_col):
        whole = whole + w2_ref[d].astype(f32)
    w4_ref[r, c] = (whole * (1.0 / total)).astype(bf16)
    for o in range(1, n_col):
        w3_copy(o).start()

    for o in range(1, half):
        source = lax.rem(pair + o, half)
        remote(
            glsum_ref.at[source], gl_ref.at[source], gls_sem.at[o], glr_sem.at[source],
            r, source * 2 + side,
        ).wait_recv()

    @pl.when(jnp.logical_not(fixed))
    def _():
        gr_hop().wait_recv()

    for o in range(1, n_col):
        source = lax.rem(c + o, n_col)
        remote(
            w4_ref.at[r, source], w4_ref.at[r, source], w3s_sem.at[o], w3r_sem.at[source],
            r, source,
        ).wait_recv()
    for o in range(1, n_row):
        w4_copy(o).start()

    grad_left = gl_ref[0].astype(f32)
    for d in range(1, half):
        grad_left = grad_left + gl_ref[d].astype(f32)
    grad_right = grfin_ref[...].astype(f32)
    keep = keep_ref[...]
    sides = jnp.concatenate([grad_left * keep, grad_right * keep], axis=1)
    grad_norm = dot_exact(sides, proj_ref[...], NT) * gain
    normed = normed_ref[...]
    slope_ref[...] = inv_ref[...] * (
        grad_norm
        - dot_exact(grad_norm, averager, NN)
        - normed * dot_exact(grad_norm * normed, averager, NN)
    )

    for o in range(1, n_row):
        source = lax.rem(r + o, n_row)
        remote(
            w4_ref.at[source], w4_ref.at[source], w4s_sem.at[o], w4r_sem.at[source], source, c
        ).wait_recv()
    gw_out_ref[...] = w4_ref[...].astype(f32).reshape(gw_out_ref.shape).astype(bf16)

    for o in range(half):
        left_copy(o).wait_send()
        gp_copy(o).wait_send()
    for o in range(1, half):
        left_relay(o).wait_send()
        gl_copy(o).wait_send()
    for o in range(1, n_col):
        w2_copy(o).wait_send()
        w3_copy(o).wait_send()
    for o in range(1, n_row):
        right_copy(o).wait_send()
        gr_copy(o).wait_send()
        w1_copy(o).wait_send()
        w4_copy(o).wait_send()

    @pl.when(jnp.logical_not(fixed))
    def _():
        right_hop().wait_send()
        gr_hop().wait_send()


def body(
    homolog_trait_tensor,
    whitening_multiplier,
    lefthand_projection,
    righthand_projection,
    result_matrix,
    result_offset,
    sequence_tallies,
    position_molecule,
    upstream_adjoint,
):
    n_row = lax.axis_size("row")
    n_col = lax.axis_size("col")
    depth_s, full = homolog_trait_tensor.shape
    embed, hidden = lefthand_projection.shape
    pair_width = result_matrix.shape[1]
    local = full // embed
    total = local * n_row * n_col
    left_extent = total // n_row
    right_extent = total // n_col
    width = local * hidden
    channels = hidden * hidden
    rows = BLOCK * right_extent
    span = BLOCK * hidden
    half = n_col // 2
    piece = channels // (n_row * n_col)

    eye = jnp.eye(local, dtype=bf16)
    projections = jnp.concatenate(
        [jnp.kron(eye, lefthand_projection), jnp.kron(eye, righthand_projection)], axis=1
    )
    vmem = pl.BlockSpec(memory_space=pltpu.VMEM)
    smem = pl.BlockSpec(memory_space=pltpu.SMEM)
    dma = pltpu.SemaphoreType.DMA
    update, slope, grad_w = pl.pallas_call(
        functools.partial(kernel, n_row, n_col, hidden, embed),
        out_shape=(
            jax.ShapeDtypeStruct((left_extent * right_extent, pair_width), bf16),
            jax.ShapeDtypeStruct((depth_s, full), f32),
            jax.ShapeDtypeStruct((channels, pair_width), bf16),
        ),
        in_specs=[vmem] * 5 + [smem] * 2 + [vmem],
        out_specs=(vmem,) * 3,
        scratch_shapes=[
            pltpu.VMEM((depth_s, full), f32),
            pltpu.VMEM((depth_s, full), f32),
            pltpu.VMEM((depth_s, width), bf16),
            pltpu.VMEM((depth_s, width), bf16),
            pltpu.VMEM((depth_s, left_extent * hidden), bf16),
            pltpu.VMEM((depth_s, right_extent * hidden), bf16),
            pltpu.VMEM((right_extent * hidden // LANES, span, LANES), f32),
            pltpu.VMEM((rows, channels), bf16),
            pltpu.VMEM((rows, pair_width), f32),
            pltpu.VMEM((left_extent * right_extent, pair_width), bf16),
            pltpu.VMEM((rows, pair_width), f32),
            pltpu.VMEM((pair_width, channels), f32),
            pltpu.VMEM((n_row, channels // n_row, pair_width), bf16),
            pltpu.VMEM((n_row, channels // n_row, pair_width), bf16),
            pltpu.VMEM((n_col, piece, pair_width), bf16),
            pltpu.VMEM((n_col, piece, pair_width), bf16),
            pltpu.VMEM((n_row, n_col, piece, pair_width), bf16),
            pltpu.VMEM((rows, channels), f32),
            pltpu.VMEM((right_extent * hidden // LANES, span, LANES), f32),
            pltpu.VMEM((depth_s, left_extent * hidden), bf16),
            pltpu.VMEM((half, depth_s, width), bf16),
            pltpu.VMEM((half, depth_s, width), bf16),
            pltpu.VMEM((half, depth_s, width), bf16),
            pltpu.VMEM((depth_s, right_extent * hidden), f32),
            pltpu.VMEM((depth_s, right_extent * hidden), bf16),
            pltpu.VMEM((n_row, depth_s, width), bf16),
            pltpu.VMEM((depth_s, width), bf16),
            pltpu.VMEM((depth_s, width), bf16),
            dma((half,)), dma((half,)), dma((n_col,)),
            dma((n_row,)), dma((n_row,)),
            dma((half,)), dma((half,)), dma((half,)), dma((half,)),
            dma((n_row,)), dma((n_row,)), dma((3,)),
            dma((n_row,)), dma((n_row,)), dma((n_col,)), dma((n_col,)),
            dma((n_col,)), dma((n_col,)), dma((n_row,)), dma((n_row,)),
            pltpu.VMEM((left_extent, right_extent * hidden), f32),
            pltpu.VMEM((depth_s, width), f32),
        ],
        compiler_params=pltpu.CompilerParams(
            collective_id=0, has_side_effects=True, vmem_limit_bytes=56 * 1024 * 1024
        ),
    )(
        homolog_trait_tensor,
        whitening_multiplier[None, :],
        projections,
        result_matrix,
        result_offset[None, :],
        sequence_tallies,
        position_molecule,
        upstream_adjoint.reshape(left_extent * right_extent, pair_width),
    )
    return update.reshape(left_extent, right_extent, pair_width), slope, grad_w.astype(f32)


def solution(mesh):
    in_specs = (P(None, ("row", "col")), P(), P(), P(), P(), P(), P(), P(), P("row", "col", None))
    out_specs = (P("row", "col", None), P(None, ("row", "col")), P())
    return jax.shard_map(body, mesh=mesh, in_specs=in_specs, out_specs=out_specs, check_vma=False)
```
